32 devices in a mesh: seq: 32 (over z, y, x, core).
Axes of the slice: x: 2, y: 2, z: 4, core: 2. Of those that a mesh axis runs over, the one named last changes fastest.
Arguments:
- values: bfloat16 [16384, 2048], P('seq'), may hold values from -6 to 6
- keys_queries: bfloat16 [16384, 128], P('seq'), may hold values from -2 to 2
- step_size: float32 [16384, 32], P('seq'), may hold values from 0.1 to 1.9
- level_logits: float32 [16384, 480], P('seq'), may hold values from -6 to 6
- decay_rate: float32 [32], replicated, may hold values from 1.2207031e-05 to 0.03
- resets: int32 [32], P('seq'), may hold values 0 or 1
Outputs:
- mixed: bfloat16 [16384, 2048], P('seq')
The draws below stay inside these ranges and needn't reach their ends.
Inputs may be any that keep to these rules, and one draw needn't show every extreme that they name: resets[b] is 1 where a document starts at the first token of block b.
All inputs are finite; a program needn't handle non-finite values.
Results may differ from the reference program's by a relative error of at most 0.0012.
The reference program's roundings to bfloat16 on the way count: a program that leaves them out, or rounds other values in their place, can miss the bound.
Values sent between devices are 32-bit elements; how exact they have to be, the bound alone decides.
A program may use at most 64 MiB of HBM per device.

```python
import math
import jax
import jax.numpy as jnp
from jax import lax

HEADS = 32
HEAD_DIM = 64
STATE = 64
TOK_DEV = 512
LEV_IN = 10
LOG_N = 5
LEVELS = 15
TOKENS = 16384
N_SEQ = 32


def place_ends(result, rng, low, largest):
    index_at = [jax.random.randint(jax.random.fold_in(rng, axis), (), 0, length) for axis, length in enumerate(result.shape)]
    longest = result.shape.index(max(result.shape))
    neighbour = index_at[:longest] + [(index_at[longest] + 1) % result.shape[longest]] + index_at[longest + 1:]
    return result.at[tuple(index_at)].set(low).at[tuple(neighbour)].set(largest)


def block_levels(stream_key, dims, shards, low, largest):
    def one(dim, blocks):
        heights = jax.random.uniform(jax.random.fold_in(jax.random.fold_in(stream_key, 6), dim), (blocks,), jnp.float32, low / len(shards), largest / len(shards))
        return jnp.repeat(jnp.exp(heights), dims[dim] // blocks).reshape((-1,) + (1,) * (len(dims) - dim - 1))

    loudness = one(*shards[0])
    for cut in shards[1:]:
        loudness = loudness * one(*cut)
    return loudness


def centred(own_key, extent, deviation, limit, shards=(), kind=jnp.bfloat16):
    drawn = deviation * jax.random.normal(own_key, extent, jnp.float32)
    if shards:
        drawn = drawn * block_levels(own_key, extent, shards, -0.22, 0.18)
    return jnp.clip(drawn, -limit, limit).astype(kind)


def setup_inputs(seed: int = 0) -> dict:
    key_list = jax.random.split(jax.random.key(seed), 7)
    values = centred(key_list[0], (TOKENS, HEADS * HEAD_DIM), 1.0, 6.0, ((0, 32),))
    keys_queries = centred(key_list[1], (TOKENS, 2 * STATE), 0.125, 2.0, ((0, 32),))
    step_size = jnp.clip(1.0 + 0.18 * jax.random.normal(key_list[2], (TOKENS, HEADS), jnp.float32), 0.1, 1.9)
    level_logits = centred(key_list[3], (TOKENS, LEVELS * HEADS), 1.0, 6.0, ((0, 32),), jnp.float32)
    decay_rate = jnp.clip(jnp.exp(jax.random.uniform(key_list[4], (HEADS,), jnp.float32, math.log(1.220703143189894e-05), math.log(0.03))), 1.220703143189894e-05, 0.03)
    resets = place_ends((jax.random.randint(key_list[5], (N_SEQ,), 0, 16) < 1).astype(jnp.int32), jax.random.fold_in(key_list[5], 1), 0, 1)
    return dict(values=values, keys_queries=keys_queries, step_size=step_size, level_logits=level_logits, decay_rate=decay_rate, resets=resets)


def level_table(length, inner_levels):
    position = jnp.arange(length, dtype=jnp.int32)
    differ = position[:, None] ^ position[None, :]
    level_map = jnp.zeros((length, length), jnp.int32)
    for power_no in range(inner_levels - 1):
        level_map = level_map + (differ >= (1 << power_no)).astype(jnp.int32)
    causal = position[:, None] >= position[None, :]
    return level_map, causal


def reference(values, keys_queries, step_size, level_logits, decay_rate, resets):
    head_count = decay_rate.shape[0]
    head_dim = values.shape[1] // head_count
    state_dim = keys_queries.shape[1] // 2
    length = TOK_DEV
    inner_levels = LEV_IN
    outer_levels = LOG_N
    block_count = N_SEQ
    level_map, causal = level_table(length, inner_levels)
    value_blocks = values.reshape(block_count, length, head_count, head_dim)
    pair_blocks = keys_queries.reshape(block_count, length, 2 * state_dim)
    step_blocks = step_size.reshape(block_count, length, head_count)
    logit_blocks = level_logits.reshape(block_count, length, LEVELS, head_count)

    def local_state(packed):
        block_values, pair_rows, step_rows = packed
        decay_sum = jnp.cumsum(-step_rows * decay_rate[None, :], axis=0)
        to_end = jnp.exp(decay_sum[-1][None, :] - decay_sum)
        decayed = (pair_rows[:, :state_dim].astype(jnp.float32).T[None] * to_end.T[:, None, :]).astype(jnp.bfloat16)
        range_state = jnp.einsum('hnl,lhp->hnp', decayed.astype(jnp.float32), block_values.astype(jnp.float32), precision=lax.Precision.HIGHEST)
        return range_state, jnp.exp(decay_sum[-1])

    block_states, block_totals = lax.map(local_state, (value_blocks, pair_blocks, step_blocks))
    entering = 1.0 - resets.astype(jnp.float32)
    factors = entering[:, None] * block_totals
    block_ids = jnp.arange(block_count, dtype=jnp.int32)

    def level_states(block_no):
        held_factor = jnp.where((block_ids < block_no)[:, None], factors, 1.0)
        inclusive = jnp.flip(jnp.cumprod(jnp.flip(held_factor, 0), 0), 0)
        through = jnp.concatenate([inclusive[1:], jnp.ones((1, head_count), jnp.float32)], 0)
        member = []
        for level_no in range(1, outer_levels + 1):
            half_span = 1 << (level_no - 1)
            middle = (block_no // half_span) * half_span
            has_level = (block_no // half_span) % 2 == 1
            member.append(((block_ids >= middle - half_span) & (block_ids < middle) & has_level).astype(jnp.float32))
        member = jnp.stack(member)
        coefficient = member[:, :, None] * through[None] * entering[block_no]
        return jnp.einsum('ljh,jhnp->lhnp', coefficient, block_states, precision=lax.Precision.HIGHEST)

    def block_output(block_no):
        states = level_states(block_no).astype(jnp.bfloat16)
        block_values = value_blocks[block_no]
        pair_rows = pair_blocks[block_no]
        key_rows = pair_rows[:, :state_dim]
        queries = pair_rows[:, state_dim:]
        decay_sum = jnp.cumsum(-step_blocks[block_no] * decay_rate[None, :], axis=0)
        weights = jax.nn.softplus(logit_blocks[block_no])
        scores = jnp.dot(queries, key_rows.T, preferred_element_type=jnp.float32)
        log_gap = decay_sum.T[:, :, None] - decay_sum.T[:, None, :]
        decays = jnp.exp(jnp.where(causal[None], log_gap, -1e30))
        level_mix = jnp.zeros((head_count, length, length), jnp.float32)
        for level_no in range(inner_levels):
            level_mix = level_mix + jnp.where(level_map[None] == level_no, weights[:, level_no, :].T[:, :, None], 0.0)
        mixing = (scores[None] * decays * level_mix).astype(jnp.bfloat16)
        local_term = jnp.einsum('hts,shp->thp', mixing.astype(jnp.float32), block_values.astype(jnp.float32), precision=lax.Precision.HIGHEST)
        scaled = jnp.exp(decay_sum)[:, None, :] * weights[:, inner_levels:, :]
        read_rows = (scaled.transpose(2, 0, 1)[:, :, :, None] * queries.astype(jnp.float32)[None, :, None, :]).astype(jnp.bfloat16)
        read_rows = read_rows.reshape(head_count, length, outer_levels * state_dim)
        stacked = states.transpose(1, 0, 2, 3).reshape(head_count, outer_levels * state_dim, head_dim)
        cross_term = jnp.einsum('htk,hkp->thp', read_rows.astype(jnp.float32), stacked.astype(jnp.float32), precision=lax.Precision.HIGHEST)
        return (local_term + cross_term).reshape(length, head_count * head_dim).astype(jnp.bfloat16)

    outputs = lax.map(block_output, block_ids)
    return outputs.reshape(block_count * length, head_count * head_dim)
```

```python
import functools

import jax
import jax.numpy as jnp
from jax import lax
from jax.experimental import pallas as pl
from jax.experimental.pallas import tpu as pltpu
from jax.sharding import PartitionSpec as P

MESH = pl.DeviceIdType.MESH
LANES = 128
CHUNKS = 4
F32 = jnp.float32
BF16 = jnp.bfloat16


def bit_length_map(differ, bits):
    out = jnp.zeros(differ.shape, jnp.int32)
    for power in range(bits):
        out = out + (differ >= (1 << power)).astype(jnp.int32)
    return out


def split3(value):
    high = value.astype(BF16)
    rest = value - high.astype(F32)
    middle = rest.astype(BF16)
    low = (rest - middle.astype(F32)).astype(BF16)
    return high, middle, low


def lanes_at(table, index):
    return jnp.take_along_axis(table, index, axis=1, mode="promise_in_bounds")


def kernel(
    count, heads, slot,
    x_ref, kq_ref, step_ref, logit_ref, rate_ref, reset_ref, out_ref,
    scores, weight, fall, ending, whole, keys_t, query2, acc, state, current, arrived,
    send_sem, recv_sem, pass_sem,
):
    length = x_ref.shape[0]
    state_dim = kq_ref.shape[1] // 2
    bits = count.bit_length() - 1
    inner = length.bit_length()
    tiles = length // LANES
    pairs = heads // 2
    half_pairs = pairs // 2
    per_chunk = half_pairs // CHUNKS
    total_row = per_chunk * state_dim
    per_group = LANES // slot
    levels = logit_ref.shape[1] // heads

    me = lax.axis_index("seq")
    core = me % 2

    def upper(bit):
        return (me // (1 << bit)) % 2

    def partner(bit):
        return me + (1 - 2 * upper(bit)) * (1 << bit)

    barrier = pltpu.get_barrier_semaphore()
    for bit in range(bits):
        pl.semaphore_signal(barrier, inc=1, device_id=(partner(bit),), device_id_type=MESH)

    steps = -(step_ref[...] * rate_ref[...])
    spread = (
        lax.broadcasted_iota(jnp.int32, (heads, LANES), 1) % heads
        == lax.broadcasted_iota(jnp.int32, (heads, LANES), 0)
    ).astype(F32).astype(BF16)
    lower = (
        lax.broadcasted_iota(jnp.int32, (length, length), 0)
        >= lax.broadcasted_iota(jnp.int32, (length, length), 1)
    ).astype(F32).astype(BF16)
    cum = jnp.zeros((length, LANES), F32)
    for part in split3(steps):
        wide = jnp.dot(part, spread, preferred_element_type=F32).astype(BF16)
        cum = cum + jnp.dot(lower, wide, preferred_element_type=F32)
    cum_t = jnp.transpose(cum)[:heads, :]
    fall[...] = jnp.exp(-cum_t)
    last = cum_t[:, length - 1:length]
    ending[...] = jnp.exp(last - cum_t)
    whole[...] = jnp.broadcast_to(jnp.exp(last), (heads, LANES))
    lane = lax.broadcasted_iota(jnp.int32, (1, LANES), 1)
    left = lane < state_dim
    pair_rows = kq_ref[...].astype(F32)
    keys_t[...] = jnp.transpose(pair_rows)[:state_dim, :]
    entering = 1.0 - reset_ref[0].astype(F32)

    pl.semaphore_wait(barrier, bits)

    def state_copy(half, chunk):
        return pltpu.make_async_remote_copy(
            src_ref=state.at[half, chunk], dst_ref=arrived.at[0, half, chunk],
            send_sem=send_sem.at[0, half, chunk], recv_sem=recv_sem.at[0, half, chunk],
            device_id=(partner(0),), device_id_type=MESH,
        )

    def range_copy(bit, chunk):
        return pltpu.make_async_remote_copy(
            src_ref=current.at[bit - 1, chunk], dst_ref=arrived.at[bit, core, chunk],
            send_sem=send_sem.at[bit, core, chunk], recv_sem=recv_sem.at[bit, core, chunk],
            device_id=(partner(bit),), device_id_type=MESH,
        )

    def pass_copy(bit, half, chunk):
        return pltpu.make_async_remote_copy(
            src_ref=arrived.at[bit, half, chunk], dst_ref=arrived.at[bit, half, chunk],
            send_sem=pass_sem.at[bit, chunk], recv_sem=recv_sem.at[bit, half, chunk],
            device_id=(partner(0),), device_id_type=MESH,
        )

    def make_state(step_no, _):
        half, chunk = step_no % 2, step_no // 2
        state[half, chunk, pl.ds(total_row, 8), :] = jnp.zeros((8, LANES), F32)
        for item in range(per_chunk):
            pair = half * half_pairs + chunk * per_chunk + item
            columns = pl.ds(pl.multiple_of(pair * LANES, LANES), LANES)
            rows = []
            for head in range(2):
                gone = ending[pl.ds(pair * 2 + head, 1), :]
                rows.append((keys_t[...] * gone).astype(BF16))
            both = jnp.dot(jnp.concatenate(rows, 0), x_ref[:, columns], preferred_element_type=F32)
            state[half, chunk, pl.ds(item * state_dim, state_dim), :] = jnp.where(
                left, both[:state_dim], both[state_dim:]
            )
            state[half, chunk, pl.ds(total_row + item, 1), :] = entering * jnp.where(
                left, whole[pl.ds(pair * 2, 1), :], whole[pl.ds(pair * 2 + 1, 1), :]
            )
        state_copy(half, chunk).start()
        return 0

    lax.fori_loop(0, 2 * CHUNKS, make_state, 0)

    turned = pltpu.roll(pair_rows, state_dim, 1)
    query2[...] = jnp.where(left, turned, pair_rows)
    width = logit_ref.shape[1]
    source = lax.broadcasted_iota(jnp.int32, (width, heads * slot), 0)
    target = lax.broadcasted_iota(jnp.int32, (width, heads * slot), 1)
    regroup = (
        (source % heads == target // slot) & (source // heads == target % slot)
    ).astype(F32).astype(BF16)
    for tile in range(tiles):
        rows = slice(tile * LANES, (tile + 1) * LANES)
        grown = jnp.exp(cum[rows])
        grown = jnp.concatenate([grown] * pl.cdiv(width, LANES), 1)[:, :width]
        logit = logit_ref[rows, :]
        soft = jnp.maximum(logit, 0.0) + jnp.log1p(jnp.exp(-jnp.abs(logit)))
        total = None
        for part in split3(soft * grown):
            term = jnp.dot(part, regroup, preferred_element_type=F32)
            total = term if total is None else total + term
        weight[rows, :] = total
    queries = jnp.where(left, turned, 0.0).astype(BF16)
    raw = lax.dot_general(
        queries, kq_ref[...], (((1,), (1,)), ((), ())), preferred_element_type=F32
    )
    scores[...] = jnp.where(
        lax.broadcasted_iota(jnp.int32, (length, length), 0)
        >= lax.broadcasted_iota(jnp.int32, (length, length), 1), raw, 0.0
    )
    row_at = lax.broadcasted_iota(jnp.int32, (LANES, LANES), 0)
    lane_at = lax.broadcasted_iota(jnp.int32, (LANES, LANES), 1)
    tile_levels = LANES.bit_length() - 1

    def on_event(bit, chunk):
        range_recv = range_copy(bit, chunk) if bit else state_copy(core, chunk)
        range_recv.wait_recv()
        if bit:
            pass_copy(bit, core, chunk).start()
        if bit == bits - 1:
            return
        own = current.at[bit - 1, chunk] if bit else state.at[core, chunk]
        is_upper = upper(bit) == 1
        mine_total = own[pl.ds(total_row, 8), :]
        other_total = arrived[bit, core, chunk, pl.ds(total_row, 8), :]
        for item in range(per_chunk):
            span = pl.ds(item * state_dim, state_dim)
            mine, other = own[span, :], arrived[bit, core, chunk, span, :]
            early = jnp.where(is_upper, other, mine)
            late = jnp.where(is_upper, mine, other)
            late_total = jnp.where(is_upper, mine_total, other_total)[item:item + 1]
            current[bit, chunk, span, :] = late + late_total * early
        current[bit, chunk, pl.ds(total_row, 8), :] = mine_total * other_total
        range_copy(bit + 1, chunk).start()

    events = {}
    for bit in range(bits):
        for chunk in range(CHUNKS):
            due = min(pairs, max(0, 1 + (bit * 5) // 2 + (chunk * 3) // 2))
            events.setdefault(due, []).append((bit, chunk))

    def local_pair(pair, _):
        for due in range(pairs):
            if due in events:
                @pl.when(pair == due)
                def _():
                    for bit, chunk in events[due]:
                        on_event(bit, chunk)
        columns = pl.ds(pl.multiple_of(pair * LANES, LANES), LANES)
        group = pl.ds(pl.multiple_of((pair * 2 // per_group) * LANES, LANES), LANES)
        base = (pair * 2 % per_group) * slot
        for tile in range(tiles):
            rows = slice(tile * LANES, (tile + 1) * LANES)
            table = weight[rows, group]
            done = []
            for head in range(2):
                first = base + head * slot
                gain = {}
                strip = []
                drop = fall[pl.ds(pair * 2 + head, 1), :]
                for past in range(tile + 1):
                    level = tile_levels + (tile ^ past).bit_length()
                    if past == tile:
                        near = bit_length_map(row_at ^ lane_at, tile_levels)
                        gain[level] = lanes_at(table, near + first)
                    elif level not in gain:
                        gain[level] = lanes_at(table, jnp.full((LANES, LANES), level, jnp.int32) + first)
                    span = slice(past * LANES, (past + 1) * LANES)
                    strip.append((scores[rows, span] * drop[:, span] * gain[level]).astype(BF16))
                strip = jnp.concatenate(strip, 1) if tile else strip[0]
                done.append(jnp.dot(
                    strip, x_ref[:(tile + 1) * LANES, columns], preferred_element_type=F32
                ))
            acc[rows, columns] = jnp.where(left, done[0], done[1])
        return 0

    lax.fori_loop(0, pairs, local_pair, 0)
    for bit, chunk in events.get(pairs, []):
        on_event(bit, chunk)

    for chunk in range(CHUNKS):
        state_copy(1 - core, chunk).wait_recv()
        for bit in range(1, bits):
            pass_copy(bit, 1 - core, chunk).wait_recv()

    couples = pl.cdiv(bits, 2)

    def cross_pair(pair, _):
        half = pair // half_pairs
        chunk = pair % half_pairs // per_chunk
        item = pair % per_chunk
        columns = pl.ds(pl.multiple_of(pair * LANES, LANES), LANES)
        group = pl.ds(pl.multiple_of((pair * 2 // per_group) * LANES, LANES), LANES)
        base = (pair * 2 % per_group) * slot
        prefix = jnp.ones((1, LANES), F32) * entering
        stack = []
        for bit in range(bits):
            is_upper = upper(bit) == 1
            other = arrived[bit, half, chunk, pl.ds(pl.multiple_of(item * state_dim, state_dim), state_dim), :]
            other_total = arrived[bit, half, chunk, pl.ds(total_row + item, 1), :]
            stack.append((other * jnp.where(is_upper, prefix, 0.0)).astype(BF16))
            prefix = jnp.where(is_upper, prefix * other_total, prefix)
        if bits % 2:
            stack.append(jnp.zeros((state_dim, LANES), BF16))
        stack = jnp.concatenate(stack, 0)
        for tile in range(tiles):
            rows = slice(tile * LANES, (tile + 1) * LANES)
            table = weight[rows, group]
            done = []
            for head in range(2):
                reads = []
                for couple in range(couples):
                    at = jnp.where(lane_at < state_dim, 0, 1) + (base + head * slot + inner + 2 * couple)
                    reads.append((lanes_at(table, at) * query2[rows, :]).astype(BF16))
                done.append(jnp.dot(jnp.concatenate(reads, 1), stack, preferred_element_type=F32))
            out_ref[rows, columns] = (
                acc[rows, columns] + jnp.where(left, done[0], done[1])
            ).astype(BF16)
        return 0

    lax.fori_loop(0, pairs, cross_pair, 0)

    for chunk in range(CHUNKS):
        for half in range(2):
            state_copy(half, chunk).wait_send()
        for bit in range(1, bits):
            range_copy(bit, chunk).wait_send()
            pass_copy(bit, core, chunk).wait_send()


def solution(mesh):
    count = mesh.shape["seq"]
    bits = count.bit_length() - 1

    def local(values, keys_queries, step_size, level_logits, decay_rate, resets):
        length, columns = values.shape
        heads = decay_rate.shape[0]
        state_dim = keys_queries.shape[1] // 2
        levels = level_logits.shape[1] // heads
        slot = 1 << levels.bit_length()
        chunk_rows = heads // 4 // CHUNKS * state_dim + 8
        vmem = pl.BlockSpec(memory_space=pltpu.VMEM)
        return pl.pallas_call(
            functools.partial(kernel, count, heads, slot),
            out_shape=jax.ShapeDtypeStruct((length, columns), values.dtype),
            in_specs=[vmem] * 5 + [pl.BlockSpec(memory_space=pltpu.SMEM)],
            out_specs=vmem,
            scratch_shapes=[
                pltpu.VMEM((length, length), F32),
                pltpu.VMEM((length, heads * slot), F32),
                pltpu.VMEM((heads, length), F32),
                pltpu.VMEM((heads, length), F32),
                pltpu.VMEM((heads, LANES), F32),
                pltpu.VMEM((state_dim, length), F32),
                pltpu.VMEM((length, 2 * state_dim), F32),
                pltpu.VMEM((length, columns), F32),
                pltpu.VMEM((2, CHUNKS, chunk_rows, LANES), F32),
                pltpu.VMEM((bits - 1, CHUNKS, chunk_rows, LANES), F32),
                pltpu.VMEM((bits, 2, CHUNKS, chunk_rows, LANES), F32),
                pltpu.SemaphoreType.DMA((bits, 2, CHUNKS)),
                pltpu.SemaphoreType.DMA((bits, 2, CHUNKS)),
                pltpu.SemaphoreType.DMA((bits, CHUNKS)),
            ],
            compiler_params=pltpu.CompilerParams(
                collective_id=0, has_side_effects=True, vmem_limit_bytes=64000000
            ),
        )(values, keys_queries, step_size, level_logits, decay_rate.reshape(1, heads), resets)

    placed = (P("seq", None), P("seq", None), P("seq", None), P("seq", None), P(), P("seq"))
    return jax.shard_map(
        local, mesh=mesh, in_specs=placed, out_specs=P("seq", None), check_vma=False
    )
```

```python
import functools

import jax
import jax.numpy as jnp
from jax import lax
from jax.experimental import pallas as pl
from jax.experimental.pallas import tpu as pltpu
from jax.sharding import PartitionSpec as P

MESH = pl.DeviceIdType.MESH
LANES = 128
CHUNKS = 4
F32 = jnp.float32
BF16 = jnp.bfloat16


def bit_length_map(differ, bits):
    out = jnp.zeros(differ.shape, jnp.int32)
    for power in range(bits):
        out = out + (differ >= (1 << power)).astype(jnp.int32)
    return out


def split3(value):
    high = value.astype(BF16)
    rest = value - high.astype(F32)
    middle = rest.astype(BF16)
    low = (rest - middle.astype(F32)).astype(BF16)
    return high, middle, low


def lanes_at(table, index):
    picks = lax.GatherDimensionNumbers(
        offset_dims=(), collapsed_slice_dims=(1,), start_index_map=(1,),
        operand_batching_dims=(0,), start_indices_batching_dims=(0,),
    )
    return lax.gather(
        table, index[..., None], picks, (1, 1), mode=lax.GatherScatterMode.PROMISE_IN_BOUNDS
    )


def kernel(
    count, heads, slot,
    x_hbm, logit_hbm, kq_ref, step_ref, rate_ref, reset_ref, out_hbm,
    x_ref, logit_ref, out_ref, final_reads,
    scores, weight, fall, ending, whole, keys_t, query2, acc, state, current, arrived,
    send_sem, recv_sem, pass_sem, in_sem, out_sem,
):
    length = x_ref.shape[0]
    state_dim = kq_ref.shape[1] // 2
    bits = count.bit_length() - 1
    inner = length.bit_length()
    tiles = length // LANES
    pairs = heads // 2
    half_pairs = pairs // 2
    per_chunk = half_pairs // CHUNKS
    total_row = per_chunk * state_dim
    per_group = LANES // slot

    me = lax.axis_index("seq")
    core = me % 2

    def upper(bit):
        return (me // (1 << bit)) % 2

    def partner(bit):
        return me + (1 - 2 * upper(bit)) * (1 << bit)

    x_load = pltpu.make_async_copy(x_hbm, x_ref, in_sem.at[0])
    logit_load = pltpu.make_async_copy(logit_hbm, logit_ref, in_sem.at[1])
    x_load.start()
    logit_load.start()
    barrier = pltpu.get_barrier_semaphore()
    for bit in range(bits):
        pl.semaphore_signal(barrier, inc=1, device_id=(partner(bit),), device_id_type=MESH)

    steps = -(step_ref[...] * rate_ref[...])
    earlier = (
        lax.broadcasted_iota(jnp.int32, (length, length), 0)
        <= lax.broadcasted_iota(jnp.int32, (length, length), 1)
    ).astype(F32).astype(BF16)
    sums = jnp.dot(jnp.concatenate(split3(steps), 0), earlier, preferred_element_type=F32)
    cum_t = sums[:heads] + sums[heads:2 * heads] + sums[2 * heads:]
    grown = jnp.exp(cum_t)
    fall[...] = jnp.exp(-cum_t)
    last = cum_t[:, length - 1:length]
    ending[...] = jnp.exp(last - cum_t)
    whole[...] = jnp.broadcast_to(jnp.exp(last), (heads, LANES))
    lane = lax.broadcasted_iota(jnp.int32, (1, LANES), 1)
    left = lane < state_dim
    pair_rows = kq_ref[...].astype(F32)
    keys_t[...] = jnp.transpose(pair_rows)[:state_dim, :]
    entering = 1.0 - reset_ref[0].astype(F32)

    pl.semaphore_wait(barrier, bits)
    x_load.wait()

    def state_copy(half, chunk):
        return pltpu.make_async_remote_copy(
            src_ref=state.at[half, chunk], dst_ref=arrived.at[0, half, chunk],
            send_sem=send_sem.at[0, half, chunk], recv_sem=recv_sem.at[0, half, chunk],
            device_id=(partner(0),), device_id_type=MESH,
        )

    def range_copy(bit, chunk):
        return pltpu.make_async_remote_copy(
            src_ref=current.at[bit - 1, chunk], dst_ref=arrived.at[bit, core, chunk],
            send_sem=send_sem.at[bit, core, chunk], recv_sem=recv_sem.at[bit, core, chunk],
            device_id=(partner(bit),), device_id_type=MESH,
        )

    def pass_copy(bit, half, chunk):
        return pltpu.make_async_remote_copy(
            src_ref=arrived.at[bit, half, chunk], dst_ref=arrived.at[bit, half, chunk],
            send_sem=pass_sem.at[bit, chunk], recv_sem=recv_sem.at[bit, half, chunk],
            device_id=(partner(0),), device_id_type=MESH,
        )

    def make_state(step_no, _):
        half, chunk = step_no % 2, step_no // 2
        state[half, chunk, pl.ds(total_row, 8), :] = jnp.zeros((8, LANES), F32)
        for item in range(per_chunk):
            pair = half * half_pairs + chunk * per_chunk + item
            columns = pl.ds(pl.multiple_of(pair * LANES, LANES), LANES)
            rows = []
            for head in range(2):
                gone = ending[pl.ds(pair * 2 + head, 1), :]
                rows.append((keys_t[...] * gone).astype(BF16))
            both = jnp.dot(jnp.concatenate(rows, 0), x_ref[:, columns], preferred_element_type=F32)
            state[half, chunk, pl.ds(item * state_dim, state_dim), :] = jnp.where(
                left, both[:state_dim], both[state_dim:]
            )
            state[half, chunk, pl.ds(total_row + item, 1), :] = entering * jnp.where(
                left, whole[pl.ds(pair * 2, 1), :], whole[pl.ds(pair * 2 + 1, 1), :]
            )
        state_copy(half, chunk).start()
        return 0

    lax.fori_loop(0, 2 * CHUNKS, make_state, 0)

    turned = pltpu.roll(pair_rows, state_dim, 1)
    query2[...] = jnp.where(left, turned, pair_rows)
    logit_load.wait()
    width = logit_ref.shape[0]
    source = lax.broadcasted_iota(jnp.int32, (width, heads * slot), 0)
    target = lax.broadcasted_iota(jnp.int32, (width, heads * slot), 1)
    regroup = (
        (source % heads == target // slot) & (source // heads == target % slot)
    ).astype(F32).astype(BF16)
    for tile in range(tiles):
        rows = slice(tile * LANES, (tile + 1) * LANES)
        logit = logit_ref[:, rows]
        soft = jnp.maximum(logit, 0.0) + jnp.log1p(jnp.exp(-jnp.abs(logit)))
        soft = soft * jnp.concatenate([grown[:, rows]] * (width // heads), 0)
        total = None
        for part in split3(soft):
            term = lax.dot_general(
                part, regroup, (((0,), (0,)), ((), ())), preferred_element_type=F32
            )
            total = term if total is None else total + term
        weight[rows, :] = total
    queries = jnp.where(left, turned, 0.0).astype(BF16)
    raw = lax.dot_general(
        queries, kq_ref[...], (((1,), (1,)), ((), ())), preferred_element_type=F32
    )
    scores[...] = jnp.where(
        lax.broadcasted_iota(jnp.int32, (length, length), 0)
        >= lax.broadcasted_iota(jnp.int32, (length, length), 1), raw, 0.0
    )
    row_at = lax.broadcasted_iota(jnp.int32, (LANES, LANES), 0)
    lane_at = lax.broadcasted_iota(jnp.int32, (LANES, LANES), 1)
    tile_levels = LANES.bit_length() - 1

    def on_event(bit, chunk):
        range_recv = range_copy(bit, chunk) if bit else state_copy(core, chunk)
        range_recv.wait_recv()
        if bit:
            pass_copy(bit, core, chunk).start()
        if bit == bits - 1:
            return
        own = current.at[bit - 1, chunk] if bit else state.at[core, chunk]
        is_upper = upper(bit) == 1
        mine_total = own[pl.ds(total_row, 8), :]
        other_total = arrived[bit, core, chunk, pl.ds(total_row, 8), :]
        for item in range(per_chunk):
            span = pl.ds(item * state_dim, state_dim)
            mine, other = own[span, :], arrived[bit, core, chunk, span, :]
            early = jnp.where(is_upper, other, mine)
            late = jnp.where(is_upper, mine, other)
            late_total = jnp.where(is_upper, mine_total, other_total)[item:item + 1]
            current[bit, chunk, span, :] = late + late_total * early
        current[bit, chunk, pl.ds(total_row, 8), :] = mine_total * other_total
        range_copy(bit + 1, chunk).start()

    events, late_events = {}, {}
    for bit in range(bits - 1):
        for chunk in range(CHUNKS):
            due = min(pairs - 1, 1 + (bit * 5) // 2 + (chunk * 3) // 2)
            events.setdefault(due, []).append((bit, chunk))
    for chunk in range(CHUNKS):
        due = min(pairs - 1, 2 + chunk * pairs // CHUNKS)
        late_events.setdefault(due, []).append((bits - 1, chunk))

    def run_events(table, pair):
        for due in table:
            @pl.when(pair == due)
            def _():
                for bit, chunk in table[due]:
                    on_event(bit, chunk)

    def local_pair(pair, _):
        run_events(events, pair)
        columns = pl.ds(pl.multiple_of(pair * LANES, LANES), LANES)
        group = pl.ds(pl.multiple_of((pair * 2 // per_group) * LANES, LANES), LANES)
        base = (pair * 2 % per_group) * slot
        for tile in range(tiles):
            rows = slice(tile * LANES, (tile + 1) * LANES)
            table = weight[rows, group]
            done = []
            for head in range(2):
                first = base + head * slot
                gain = {}
                strip = []
                drop = fall[pl.ds(pair * 2 + head, 1), :]
                for past in range(tile + 1):
                    level = tile_levels + (tile ^ past).bit_length()
                    if past == tile:
                        near = bit_length_map(row_at ^ lane_at, tile_levels)
                        gain[level] = lanes_at(table, near + first)
                    elif level not in gain:
                        at = jnp.full((1, LANES), level, jnp.int32) + first
                        gain[level] = lanes_at(table, jnp.broadcast_to(at, (LANES, LANES)))
                    span = slice(past * LANES, (past + 1) * LANES)
                    strip.append((scores[rows, span] * drop[:, span] * gain[level]).astype(BF16))
                strip = jnp.concatenate(strip, 1) if tile else strip[0]
                done.append(jnp.dot(
                    strip, x_ref[:(tile + 1) * LANES, columns], preferred_element_type=F32
                ))
            acc[rows, columns] = jnp.where(left, done[0], done[1])
        return 0

    lax.fori_loop(0, pairs, local_pair, 0)

    for chunk in range(CHUNKS):
        state_copy(1 - core, chunk).wait_recv()
        for bit in range(1, bits - 1):
            pass_copy(bit, 1 - core, chunk).wait_recv()

    def level_blocks(half, chunk, item, first, end):
        prefix = jnp.ones((1, LANES), F32) * entering
        blocks = []
        for bit in range(end):
            is_upper = upper(bit) == 1
            if bit >= first:
                other = arrived[bit, half, chunk, pl.ds(pl.multiple_of(item * state_dim, state_dim), state_dim), :]
                level = other * jnp.where(is_upper, prefix, 0.0)
                blocks.append(jnp.where(left, level, 0.0).astype(BF16))
                blocks.append(jnp.where(left, 0.0, level).astype(BF16))
            if bit < end - 1:
                other_total = arrived[bit, half, chunk, pl.ds(total_row + item, 1), :]
                prefix = jnp.where(is_upper, prefix * other_total, prefix)
        return jnp.concatenate(blocks, 0)

    def early_pair(pair, _):
        run_events(late_events, pair)
        half = pair // half_pairs
        chunk = pair % half_pairs // per_chunk
        item = pair % per_chunk
        columns = pl.ds(pl.multiple_of(pair * LANES, LANES), LANES)
        group = pl.ds(pl.multiple_of((pair * 2 // per_group) * LANES, LANES), LANES)
        base = (pair * 2 % per_group) * slot
        stack = level_blocks(half, chunk, item, 0, bits - 1)
        for tile in range(tiles):
            rows = slice(tile * LANES, (tile + 1) * LANES)
            table = weight[rows, group]
            reads = []
            for bit in range(bits):
                at = jnp.where(left, 0, slot) + (base + inner + bit)
                gain = lanes_at(table, jnp.broadcast_to(at, (LANES, LANES)))
                reads.append((gain * query2[rows, :]).astype(BF16))
            final_reads[rows, columns] = reads.pop()
            acc[rows, columns] += jnp.dot(
                jnp.concatenate(reads, 1), stack, preferred_element_type=F32
            )
        return 0

    lax.fori_loop(0, pairs, early_pair, 0)

    def out_copy(pair):
        columns = pl.ds(pl.multiple_of(pair * LANES, LANES), LANES)
        return pltpu.make_async_copy(
            out_ref.at[:, columns], out_hbm.at[:, columns], out_sem.at[pair]
        )

    def final_chunk(chunk, _):
        pass_copy(bits - 1, 1 - core, chunk).wait_recv()

        def final_pair(number, _):
            half, item = number // per_chunk, number % per_chunk
            pair = half * half_pairs + chunk * per_chunk + item
            columns = pl.ds(pl.multiple_of(pair * LANES, LANES), LANES)
            stack = level_blocks(half, chunk, item, bits - 1, bits)
            out_ref[:, columns] = (
                acc[:, columns]
                + jnp.dot(final_reads[:, columns], stack, preferred_element_type=F32)
            ).astype(BF16)
            out_copy(pair).start()
            return 0

        return lax.fori_loop(0, 2 * per_chunk, final_pair, 0)

    lax.fori_loop(0, CHUNKS, final_chunk, 0)

    lax.fori_loop(0, pairs, lambda pair, _: (out_copy(pair).wait(), 0)[1], 0)
    for chunk in range(CHUNKS):
        for half in range(2):
            state_copy(half, chunk).wait_send()
        for bit in range(1, bits):
            range_copy(bit, chunk).wait_send()
            pass_copy(bit, core, chunk).wait_send()


def solution(mesh):
    count = mesh.shape["seq"]
    bits = count.bit_length() - 1

    def local(values, keys_queries, step_size, level_logits, decay_rate, resets):
        length, columns = values.shape
        heads = decay_rate.shape[0]
        state_dim = keys_queries.shape[1] // 2
        levels = level_logits.shape[1] // heads
        slot = 1 << levels.bit_length()
        chunk_rows = heads // 4 // CHUNKS * state_dim + 8
        vmem = pl.BlockSpec(memory_space=pltpu.VMEM)
        any_space = pl.BlockSpec(memory_space=pl.ANY)
        return pl.pallas_call(
            functools.partial(kernel, count, heads, slot),
            out_shape=jax.ShapeDtypeStruct((length, columns), values.dtype),
            in_specs=[any_space] * 2 + [vmem] * 3 + [pl.BlockSpec(memory_space=pltpu.SMEM)],
            out_specs=any_space,
            scratch_shapes=[
                pltpu.VMEM((length, columns), BF16),
                pltpu.VMEM((levels * heads, length), F32),
                pltpu.VMEM((length, columns), BF16),
                pltpu.VMEM((length, columns), BF16),
                pltpu.VMEM((length, length), F32),
                pltpu.VMEM((length, heads * slot), F32),
                pltpu.VMEM((heads, length), F32),
                pltpu.VMEM((heads, length), F32),
                pltpu.VMEM((heads, LANES), F32),
                pltpu.VMEM((state_dim, length), F32),
                pltpu.VMEM((length, 2 * state_dim), F32),
                pltpu.VMEM((length, columns), F32),
                pltpu.VMEM((2, CHUNKS, chunk_rows, LANES), F32),
                pltpu.VMEM((bits - 1, CHUNKS, chunk_rows, LANES), F32),
                pltpu.VMEM((bits, 2, CHUNKS, chunk_rows, LANES), F32),
                pltpu.SemaphoreType.DMA((bits, 2, CHUNKS)),
                pltpu.SemaphoreType.DMA((bits, 2, CHUNKS)),
                pltpu.SemaphoreType.DMA((bits, CHUNKS)),
                pltpu.SemaphoreType.DMA((2,)),
                pltpu.SemaphoreType.DMA((heads // 2,)),
            ],
            compiler_params=pltpu.CompilerParams(
                collective_id=0, has_side_effects=True, vmem_limit_bytes=64000000
            ),
        )(values, level_logits.T, keys_queries, step_size.T, decay_rate.reshape(heads, 1), resets)

    placed = (P("seq", None), P("seq", None), P("seq", None), P("seq", None), P(), P("seq"))
    return jax.shard_map(
        local, mesh=mesh, in_specs=placed, out_specs=P("seq", None), check_vma=False
    )
```

```python
import functools

import jax
import jax.numpy as jnp
from jax import lax
from jax.experimental import pallas as pl
from jax.experimental.pallas import tpu as pltpu
from jax.sharding import PartitionSpec as P

MESH = pl.DeviceIdType.MESH
LANES = 128
SCALE = 1.5
PREP = 5.0
LATE = 4
CHUNKS = 4
F32 = jnp.float32
BF16 = jnp.bfloat16


def bit_length_map(differ, bits):
    out = jnp.zeros(differ.shape, jnp.int32)
    for power in range(bits):
        out = out + (differ >= (1 << power)).astype(jnp.int32)
    return out


def split3(value):
    high = value.astype(BF16)
    rest = value - high.astype(F32)
    middle = rest.astype(BF16)
    low = (rest - middle.astype(F32)).astype(BF16)
    return high, middle, low


def lanes_at(table, index):
    picks = lax.GatherDimensionNumbers(
        offset_dims=(), collapsed_slice_dims=(1,), start_index_map=(1,),
        operand_batching_dims=(0,), start_indices_batching_dims=(0,),
    )
    return lax.gather(
        table, index[..., None], picks, (1, 1), mode=lax.GatherScatterMode.PROMISE_IN_BOUNDS
    )


def kernel(
    count, heads, slot,
    x_hbm, logit_hbm, kq_ref, step_ref, rate_ref, reset_ref, out_hbm,
    x_ref, logit_ref, out_ref, final_reads,
    scores, weight, fall, ending, whole, keys_t, query2, acc, state, current, arrived,
    send_sem, recv_sem, pass_sem, in_sem, out_sem,
):
    length = x_ref.shape[0]
    state_dim = kq_ref.shape[1] // 2
    bits = count.bit_length() - 1
    inner = length.bit_length()
    tiles = length // LANES
    pairs = heads // 2
    half_pairs = pairs // 2
    per_chunk = half_pairs // CHUNKS
    total_row = per_chunk * state_dim
    per_group = LANES // slot

    me = lax.axis_index("seq")
    core = me % 2

    def upper(bit):
        return (me // (1 << bit)) % 2

    def partner(bit):
        return me + (1 - 2 * upper(bit)) * (1 << bit)

    x_load = pltpu.make_async_copy(x_hbm, x_ref, in_sem.at[0])
    logit_load = pltpu.make_async_copy(logit_hbm, logit_ref, in_sem.at[1])
    x_load.start()
    logit_load.start()
    barrier = pltpu.get_barrier_semaphore()
    for bit in range(bits):
        pl.semaphore_signal(barrier, inc=1, device_id=(partner(bit),), device_id_type=MESH)

    diagonal = (
        lax.broadcasted_iota(jnp.int32, (heads, heads), 0)
        == lax.broadcasted_iota(jnp.int32, (heads, heads), 1)
    )
    rates = jnp.sum(jnp.where(diagonal, rate_ref[...], 0.0), axis=1, keepdims=True)
    steps = -(step_ref[...] * rates)
    earlier = (
        lax.broadcasted_iota(jnp.int32, (length, length), 0)
        <= lax.broadcasted_iota(jnp.int32, (length, length), 1)
    ).astype(F32).astype(BF16)
    sums = jnp.dot(jnp.concatenate(split3(steps), 0), earlier, preferred_element_type=F32)
    cum_t = sums[:heads] + sums[heads:2 * heads] + sums[2 * heads:]
    grown = jnp.exp(cum_t)
    fall[...] = jnp.exp(-cum_t)
    last = cum_t[:, length - 1:length]
    ending[...] = jnp.exp(last - cum_t)
    whole[...] = jnp.broadcast_to(jnp.exp(last), (heads, LANES))
    lane = lax.broadcasted_iota(jnp.int32, (1, LANES), 1)
    left = lane < state_dim
    pair_rows = kq_ref[...].astype(F32)
    keys_t[...] = jnp.transpose(pair_rows)[:state_dim, :]
    entering = 1.0 - reset_ref[0].astype(F32)

    pl.semaphore_wait(barrier, bits)
    x_load.wait()

    def state_copy(half, chunk):
        return pltpu.make_async_remote_copy(
            src_ref=state.at[half, chunk], dst_ref=arrived.at[0, half, chunk],
            send_sem=send_sem.at[0, half, chunk], recv_sem=recv_sem.at[0, half, chunk],
            device_id=(partner(0),), device_id_type=MESH,
        )

    def range_copy(bit, chunk):
        return pltpu.make_async_remote_copy(
            src_ref=current.at[bit - 1, chunk], dst_ref=arrived.at[bit, core, chunk],
            send_sem=send_sem.at[bit, core, chunk], recv_sem=recv_sem.at[bit, core, chunk],
            device_id=(partner(bit),), device_id_type=MESH,
        )

    def pass_copy(bit, half, chunk):
        return pltpu.make_async_remote_copy(
            src_ref=arrived.at[bit, half, chunk], dst_ref=arrived.at[bit, half, chunk],
            send_sem=pass_sem.at[bit, chunk], recv_sem=recv_sem.at[bit, half, chunk],
            device_id=(partner(0),), device_id_type=MESH,
        )

    def make_state(step_no, _):
        half, chunk = step_no % 2, step_no // 2
        state[half, chunk, pl.ds(total_row, 8), :] = jnp.zeros((8, LANES), F32)
        for item in range(per_chunk):
            pair = half * half_pairs + chunk * per_chunk + item
            columns = pl.ds(pl.multiple_of(pair * LANES, LANES), LANES)
            rows = []
            for head in range(2):
                gone = ending[pl.ds(pair * 2 + head, 1), :]
                rows.append((keys_t[...] * gone).astype(BF16))
            both = jnp.dot(jnp.concatenate(rows, 0), x_ref[:, columns], preferred_element_type=F32)
            state[half, chunk, pl.ds(item * state_dim, state_dim), :] = jnp.where(
                left, both[:state_dim], both[state_dim:]
            )
            state[half, chunk, pl.ds(total_row + item, 1), :] = entering * jnp.where(
                left, whole[pl.ds(pair * 2, 1), :], whole[pl.ds(pair * 2 + 1, 1), :]
            )
        state_copy(half, chunk).start()
        return 0

    lax.fori_loop(0, 2 * CHUNKS, make_state, 0)

    prep_events, events, late_events = {}, {}, {}
    for bit in range(1, bits - 1):
        for chunk in range(CHUNKS):
            due = SCALE * (3.0 + 3.2 * (bit - 1) + 1.5 * chunk)
            if due < PREP:
                prep_events.setdefault(int(due * tiles / PREP), []).append((bit, chunk))
            else:
                due = min(pairs - 1, int((due - PREP) / 0.8))
                events.setdefault(due, []).append((bit, chunk))
    for chunk in range(CHUNKS):
        due = min(pairs - 1, LATE + chunk * pairs // (CHUNKS + 1))
        late_events.setdefault(due, []).append((bits - 1, chunk))
    def on_event(bit, chunk):
        range_recv = range_copy(bit, chunk) if bit else state_copy(core, chunk)
        range_recv.wait_recv()
        if bit:
            pass_copy(bit, core, chunk).start()
        if bit == bits - 1:
            return
        own = current.at[bit - 1, chunk] if bit else state.at[core, chunk]
        is_upper = upper(bit) == 1
        mine_total = own[pl.ds(total_row, 8), :]
        other_total = arrived[bit, core, chunk, pl.ds(total_row, 8), :]
        for item in range(per_chunk):
            span = pl.ds(item * state_dim, state_dim)
            mine, other = own[span, :], arrived[bit, core, chunk, span, :]
            early = jnp.where(is_upper, other, mine)
            late = jnp.where(is_upper, mine, other)
            late_total = jnp.where(is_upper, mine_total, other_total)[item:item + 1]
            current[bit, chunk, span, :] = late + late_total * early
        current[bit, chunk, pl.ds(total_row, 8), :] = mine_total * other_total
        range_copy(bit + 1, chunk).start()

    for chunk in range(CHUNKS):
        on_event(0, chunk)

    turned = pltpu.roll(pair_rows, state_dim, 1)
    query2[...] = jnp.where(left, turned, pair_rows)
    logit_load.wait()
    width = logit_ref.shape[0]
    source = lax.broadcasted_iota(jnp.int32, (width, heads * slot), 0)
    target = lax.broadcasted_iota(jnp.int32, (width, heads * slot), 1)
    regroup = (
        (source % heads == target // slot) & (source // heads == target % slot)
    ).astype(F32).astype(BF16)
    for tile in range(tiles):
        rows = slice(tile * LANES, (tile + 1) * LANES)
        logit = logit_ref[:, rows]
        soft = jnp.maximum(logit, 0.0) + jnp.log1p(jnp.exp(-jnp.abs(logit)))
        soft = soft * jnp.concatenate([grown[:, rows]] * (width // heads), 0)
        total = None
        for part in split3(soft):
            term = lax.dot_general(
                part, regroup, (((0,), (0,)), ((), ())), preferred_element_type=F32
            )
            total = term if total is None else total + term
        weight[rows, :] = total
        for bit, chunk in prep_events.get(tile, []):
            on_event(bit, chunk)
    queries = jnp.where(left, turned, 0.0).astype(BF16)
    raw = lax.dot_general(
        queries, kq_ref[...], (((1,), (1,)), ((), ())), preferred_element_type=F32
    )
    scores[...] = jnp.where(
        lax.broadcasted_iota(jnp.int32, (length, length), 0)
        >= lax.broadcasted_iota(jnp.int32, (length, length), 1), raw, 0.0
    )
    row_at = lax.broadcasted_iota(jnp.int32, (LANES, LANES), 0)
    lane_at = lax.broadcasted_iota(jnp.int32, (LANES, LANES), 1)
    tile_levels = LANES.bit_length() - 1

    def run_events(table, pair):
        for due in table:
            @pl.when(pair == due)
            def _():
                for bit, chunk in table[due]:
                    on_event(bit, chunk)

    def local_pair(pair, _):
        run_events(events, pair)
        columns = pl.ds(pl.multiple_of(pair * LANES, LANES), LANES)
        group = pl.ds(pl.multiple_of((pair * 2 // per_group) * LANES, LANES), LANES)
        base = (pair * 2 % per_group) * slot
        for tile in range(tiles):
            rows = slice(tile * LANES, (tile + 1) * LANES)
            table = weight[rows, group]
            done = []
            for head in range(2):
                first = base + head * slot
                gain = {}
                strip = []
                drop = fall[pl.ds(pair * 2 + head, 1), :]
                for past in range(tile + 1):
                    level = tile_levels + (tile ^ past).bit_length()
                    if past == tile:
                        near = bit_length_map(row_at ^ lane_at, tile_levels)
                        gain[level] = lanes_at(table, near + first)
                    elif level not in gain:
                        at = jnp.full((1, LANES), level, jnp.int32) + first
                        gain[level] = lanes_at(table, jnp.broadcast_to(at, (LANES, LANES)))
                    span = slice(past * LANES, (past + 1) * LANES)
                    strip.append((scores[rows, span] * drop[:, span] * gain[level]).astype(BF16))
                strip = jnp.concatenate(strip, 1) if tile else strip[0]
                done.append(jnp.dot(
                    strip, x_ref[:(tile + 1) * LANES, columns], preferred_element_type=F32
                ))
            acc[rows, columns] = jnp.where(left, done[0], done[1])
        return 0

    lax.fori_loop(0, pairs, local_pair, 0)

    for chunk in range(CHUNKS):
        state_copy(1 - core, chunk).wait_recv()
        for bit in range(1, bits - 1):
            pass_copy(bit, 1 - core, chunk).wait_recv()

    def level_blocks(half, chunk, item, first, end):
        prefix = jnp.ones((1, LANES), F32) * entering
        blocks = []
        for bit in range(end):
            is_upper = upper(bit) == 1
            if bit >= first:
                other = arrived[bit, half, chunk, pl.ds(pl.multiple_of(item * state_dim, state_dim), state_dim), :]
                level = other * jnp.where(is_upper, prefix, 0.0)
                blocks.append(jnp.where(left, level, 0.0).astype(BF16))
                blocks.append(jnp.where(left, 0.0, level).astype(BF16))
            if bit < end - 1:
                other_total = arrived[bit, half, chunk, pl.ds(total_row + item, 1), :]
                prefix = jnp.where(is_upper, prefix * other_total, prefix)
        return jnp.concatenate(blocks, 0)

    def early_pair(pair, _):
        run_events(late_events, pair)
        half = pair // half_pairs
        chunk = pair % half_pairs // per_chunk
        item = pair % per_chunk
        columns = pl.ds(pl.multiple_of(pair * LANES, LANES), LANES)
        group = pl.ds(pl.multiple_of((pair * 2 // per_group) * LANES, LANES), LANES)
        base = (pair * 2 % per_group) * slot
        stack = level_blocks(half, chunk, item, 0, bits - 1)
        for tile in range(tiles):
            rows = slice(tile * LANES, (tile + 1) * LANES)
            table = weight[rows, group]
            reads = []
            for bit in range(bits):
                at = jnp.where(left, 0, slot) + (base + inner + bit)
                gain = lanes_at(table, jnp.broadcast_to(at, (LANES, LANES)))
                reads.append((gain * query2[rows, :]).astype(BF16))
            final_reads[rows, columns] = reads.pop()
            acc[rows, columns] += jnp.dot(
                jnp.concatenate(reads, 1), stack, preferred_element_type=F32
            )
        return 0

    lax.fori_loop(0, pairs, early_pair, 0)

    def out_copy(pair):
        columns = pl.ds(pl.multiple_of(pair * LANES, LANES), LANES)
        return pltpu.make_async_copy(
            out_ref.at[:, columns], out_hbm.at[:, columns], out_sem.at[pair]
        )

    def final_chunk(chunk, _):
        pass_copy(bits - 1, 1 - core, chunk).wait_recv()

        def final_pair(number, _):
            half, item = number // per_chunk, number % per_chunk
            pair = half * half_pairs + chunk * per_chunk + item
            columns = pl.ds(pl.multiple_of(pair * LANES, LANES), LANES)
            stack = level_blocks(half, chunk, item, bits - 1, bits)
            out_ref[:, columns] = (
                acc[:, columns]
                + jnp.dot(final_reads[:, columns], stack, preferred_element_type=F32)
            ).astype(BF16)
            out_copy(pair).start()
            return 0

        return lax.fori_loop(0, 2 * per_chunk, final_pair, 0)

    lax.fori_loop(0, CHUNKS, final_chunk, 0)

    lax.fori_loop(0, pairs, lambda pair, _: (out_copy(pair).wait(), 0)[1], 0)
    for chunk in range(CHUNKS):
        for half in range(2):
            state_copy(half, chunk).wait_send()
        for bit in range(1, bits):
            range_copy(bit, chunk).wait_send()
            pass_copy(bit, core, chunk).wait_send()


def solution(mesh):
    count = mesh.shape["seq"]
    bits = count.bit_length() - 1

    def local(values, keys_queries, step_size, level_logits, decay_rate, resets):
        length, columns = values.shape
        heads = decay_rate.shape[0]
        state_dim = keys_queries.shape[1] // 2
        levels = level_logits.shape[1] // heads
        slot = 1 << levels.bit_length()
        chunk_rows = heads // 4 // CHUNKS * state_dim + 8
        vmem = pl.BlockSpec(memory_space=pltpu.VMEM)
        any_space = pl.BlockSpec(memory_space=pl.ANY)
        return pl.pallas_call(
            functools.partial(kernel, count, heads, slot),
            out_shape=jax.ShapeDtypeStruct((length, columns), values.dtype),
            in_specs=[any_space] * 2 + [vmem] * 3 + [pl.BlockSpec(memory_space=pltpu.SMEM)],
            out_specs=any_space,
            scratch_shapes=[
                pltpu.VMEM((length, columns), BF16),
                pltpu.VMEM((levels * heads, length), F32),
                pltpu.VMEM((length, columns), BF16),
                pltpu.VMEM((length, columns), BF16),
                pltpu.VMEM((length, length), F32),
                pltpu.VMEM((length, heads * slot), F32),
                pltpu.VMEM((heads, length), F32),
                pltpu.VMEM((heads, length), F32),
                pltpu.VMEM((heads, LANES), F32),
                pltpu.VMEM((state_dim, length), F32),
                pltpu.VMEM((length, 2 * state_dim), F32),
                pltpu.VMEM((length, columns), F32),
                pltpu.VMEM((2, CHUNKS, chunk_rows, LANES), F32),
                pltpu.VMEM((bits - 1, CHUNKS, chunk_rows, LANES), F32),
                pltpu.VMEM((bits, 2, CHUNKS, chunk_rows, LANES), F32),
                pltpu.SemaphoreType.DMA((bits, 2, CHUNKS)),
                pltpu.SemaphoreType.DMA((bits, 2, CHUNKS)),
                pltpu.SemaphoreType.DMA((bits, CHUNKS)),
                pltpu.SemaphoreType.DMA((2,)),
                pltpu.SemaphoreType.DMA((heads // 2,)),
            ],
            compiler_params=pltpu.CompilerParams(
                collective_id=0, has_side_effects=True, vmem_limit_bytes=64000000
            ),
        )(values, level_logits.T, keys_queries, step_size.T, decay_rate.reshape(1, heads), resets)

    placed = (P("seq", None), P("seq", None), P("seq", None), P("seq", None), P(), P("seq"))
    return jax.shard_map(
        local, mesh=mesh, in_specs=placed, out_specs=P("seq", None), check_vma=False
    )
```
